128 devices in a mesh: seq: 64 (over x, z, y), head: 2 (over core).
Axes of the slice: x: 4, y: 4, z: 4, core: 2. Of those that a mesh axis runs over, the one named last changes fastest.
Arguments:
- queries: bfloat16 [16384, 4096], P('seq', 'head'), may hold values from -210 to 210
- keys: bfloat16 [16384, 1024], P('seq', 'head'), may hold values from -7 to 7
- values: bfloat16 [16384, 1024], P('seq', 'head'), may hold values from -6 to 6
- vertical: int32 [8, 64], P('head'), may hold values from 0 to 255, as said below
- slash: int32 [8, 2], P('head'), may hold values from 1 to 4, as said below
- out_weight: bfloat16 [4096, 4096], P('head'), may hold values from -1 to 1
Outputs:
- mixed: bfloat16 [16384, 4096], P(('seq', 'head'))
The draws below stay inside these ranges and needn't reach their ends.
Inputs may be any that keep to these rules, and one draw needn't show every extreme that they name: `vertical`: for each key-value head, 64 different key blocks in increasing order; block b lies in slab b // 4; no slab holds more than 2 of one head's blocks, and for every head some slab holds exactly 2. `slash`: for each key-value head, 2 different offsets in increasing order; some head has the offset 256 // 64.
All inputs are finite; a program needn't handle non-finite values.
Results may differ from the reference program's by a relative error of at most 0.01.
Values may be sent and summed in bfloat16 or wider, within the bound.
A program may use at most 128 MiB of HBM per device.

```python
from functools import partial
import jax
import jax.numpy as jnp
from jax import lax

HEADS = 32
KEY_VALUE_HEADS = 8
HEAD_DIM = 128
DMODEL = 4096
S_DEV = 256
BLK = 64
NS = 2
CAP = 2
NV = 64
SEQ = 16384
N_SEQ = 64


def paired(key):
    key_seed, query_seed = jax.random.split(jax.random.fold_in(key, 7), 2)
    keys_f = jnp.clip(jax.random.normal(key_seed, (SEQ, KEY_VALUE_HEADS * HEAD_DIM), jnp.float32), -6.0, 6.0)
    query_f = jnp.clip(1.5 * jax.random.normal(query_seed, (SEQ, HEADS * HEAD_DIM), jnp.float32), -9.0, 9.0)
    return (query_f, keys_f)


def draw_queries(key, part):
    return paired(key)[0].astype(jnp.bfloat16)


def draw_keys(key, part):
    return paired(key)[1].astype(jnp.bfloat16)


def draw_vertical(key, part):
    block_span = S_DEV // BLK
    owners = SEQ // S_DEV
    perm_seed, score_seed, force_seed = jax.random.split(jax.random.fold_in(key, 3), 3)
    within = jax.random.randint(perm_seed, (KEY_VALUE_HEADS, owners, block_span), 0, 1 << 20) * block_span + jnp.arange(block_span, dtype=jnp.int32)
    order = jnp.argsort(within, axis=-1)[:, :, :CAP]
    blocks = (order + jnp.arange(owners, dtype=jnp.int32)[None, :, None] * block_span).reshape(KEY_VALUE_HEADS, owners * CAP)
    owner_of = jnp.repeat(jnp.arange(owners, dtype=jnp.int32), CAP)
    forced_blocks = jax.random.randint(force_seed, (KEY_VALUE_HEADS, 1), 0, owners)
    block_score = jax.random.randint(score_seed, (KEY_VALUE_HEADS, owners * CAP), 0, 4096) + (owners - owner_of)[None, :] * (8192 // owners)
    block_score = block_score + jnp.where(owner_of[None, :] == forced_blocks, 1 << 16, 0)
    block_score = block_score * (owners * CAP) + jnp.arange(owners * CAP, dtype=jnp.int32)[None, :]
    unused, picked = lax.top_k(block_score, NV)
    chosen = jnp.take_along_axis(blocks, picked, axis=1)
    return jnp.sort(chosen, axis=1).astype(jnp.int32)


def draw_slash(key, part):
    block_span = S_DEV // BLK
    score_seed, force_seed = jax.random.split(jax.random.fold_in(key, 5), 2)
    block_score = jax.random.randint(score_seed, (KEY_VALUE_HEADS, block_span), 0, 4096) * block_span + jnp.arange(block_span, dtype=jnp.int32)[None, :]
    forced_blocks = jax.random.randint(force_seed, (), 0, KEY_VALUE_HEADS)
    extra_score = (jnp.arange(KEY_VALUE_HEADS)[:, None] == forced_blocks) & (jnp.arange(block_span)[None, :] == block_span - 1)
    block_score = block_score + jnp.where(extra_score, 1 << 24, 0)
    unused, picked = lax.top_k(block_score, NS)
    return jnp.sort(picked + 1, axis=1).astype(jnp.int32)


def block_scale(key, shape, pieces, least, top_value):
    def one(position, blocks):
        steps = jax.random.uniform(jax.random.fold_in(jax.random.fold_in(key, 6), position), (blocks,), jnp.float32, least / len(pieces), top_value / len(pieces))
        return jnp.repeat(jnp.exp(steps), shape[position] // blocks).reshape((-1,) + (1,) * (len(shape) - position - 1))

    loudness = one(*pieces[0])
    for cut in pieces[1:]:
        loudness = loudness * one(*cut)
    return loudness


def bell_draw(key, shape, scale, bound, pieces=(), held_as=jnp.bfloat16):
    factor_of = block_scale(key, shape, pieces, -0.22, 0.18) if pieces else 1.0
    array = jax.random.normal(key, shape, jnp.float32) * scale * factor_of
    return jnp.minimum(jnp.maximum(array, -bound), bound).astype(held_as)


def setup_inputs(seed: int = 0) -> dict:
    splits = jax.random.split(jax.random.key(seed), 7)
    return {
        "queries": draw_queries(jax.random.fold_in(splits[6], 71), 0),
        "keys": draw_keys(jax.random.fold_in(splits[6], 71), 0),
        "values": bell_draw(splits[2], (SEQ, KEY_VALUE_HEADS * HEAD_DIM), 1.0, 6.0, ((0, 64), (1, 2))),
        "vertical": draw_vertical(jax.random.fold_in(splits[6], 71), 0),
        "slash": draw_slash(jax.random.fold_in(splits[6], 71), 0),
        "out_weight": bell_draw(splits[5], (HEADS * HEAD_DIM, DMODEL), HEADS ** -0.5, 1.0, ((0, 2),)),
    }


NEGATIVE = -1e30


def attended_block_tile(block_index, vert_ids, slash_ids, key_head, value_head, query_head_index, causal):
    offsets = jnp.concatenate([jnp.zeros((1,), jnp.int32), slash_ids.astype(jnp.int32)])
    diagonal = block_index - offsets
    vert_ok = (vert_ids < block_index) & jnp.all(block_index - vert_ids[:, None] != slash_ids[None, :], axis=1)
    diag_ok = diagonal >= 0
    chosen = jnp.concatenate([vert_ids.astype(jnp.int32), jnp.maximum(diagonal, 0).astype(jnp.int32)])
    usable = jnp.concatenate([vert_ok, diag_ok])
    gathered_keys = key_head[chosen].reshape(-1, HEAD_DIM)
    gathered_values = value_head[chosen].reshape(-1, HEAD_DIM)
    same_block = chosen == block_index
    allowed = usable[None, :, None] & (jnp.logical_not(same_block)[None, :, None] | causal[:, None, :])
    allowed = allowed.reshape(BLK, -1)
    query_block_tile = query_head_index[block_index]
    scores = jnp.einsum("qgd,kd->gqk", query_block_tile.astype(jnp.float32), gathered_keys.astype(jnp.float32)) * (HEAD_DIM ** -0.5)
    scores = jnp.where(allowed[None], scores, NEGATIVE)
    top_score = jnp.max(scores, axis=-1, keepdims=True)
    weights = jnp.where(allowed[None], jnp.exp(scores - top_score), 0.0)
    sum_weight = jnp.sum(weights, axis=-1, keepdims=True)
    rounded = lax.optimization_barrier(weights.astype(jnp.bfloat16)).astype(jnp.float32)
    output = jnp.einsum("gqk,kd->gqd", rounded, gathered_values.astype(jnp.float32)) / sum_weight
    return output.transpose(1, 0, 2).astype(jnp.bfloat16)


def attend_slab(slab_start, block_fn, slab_blocks):
    return jax.vmap(block_fn)(slab_start + jnp.arange(slab_blocks, dtype=jnp.int32))


def reference(queries, keys, values, vertical, slash, out_weight):
    per_group = HEADS // KEY_VALUE_HEADS
    block_count = SEQ // BLK
    slab_blocks = S_DEV // BLK
    query_blocks = queries.reshape(block_count, BLK, KEY_VALUE_HEADS, per_group, HEAD_DIM)
    key_blocks = keys.reshape(block_count, BLK, KEY_VALUE_HEADS, HEAD_DIM)
    value_blocks = values.reshape(block_count, BLK, KEY_VALUE_HEADS, HEAD_DIM)
    within = jnp.arange(BLK)
    causal = within[None, :] <= within[:, None]
    results = []
    for head_index in range(KEY_VALUE_HEADS):
        block_fn = partial(attended_block_tile, vert_ids=vertical[head_index], slash_ids=slash[head_index],
                           key_head=key_blocks[:, :, head_index], value_head=value_blocks[:, :, head_index],
                           query_head_index=query_blocks[:, :, head_index], causal=causal)
        mapped = lax.map(partial(attend_slab, block_fn=block_fn, slab_blocks=slab_blocks),
                         jnp.arange(N_SEQ, dtype=jnp.int32) * slab_blocks)
        results.append(mapped.reshape(SEQ, per_group * HEAD_DIM))
    attention = jnp.concatenate(results, axis=1)
    return jnp.dot(attention, out_weight, preferred_element_type=jnp.float32).astype(jnp.bfloat16)
```

```python
import functools
import math

import jax
import jax.numpy as jnp
from jax import lax
from jax.experimental import pallas as pl
from jax.experimental.pallas import tpu as pltpu
from jax.sharding import PartitionSpec as P

D = 128
BLK = 64
CAP = 2
KVL = 4
G = 4
ROWS = 256
NB = 4
RING = 4
PLANE = 16
NV = 64
OUT = 4096
NEG = -1e30
C2 = D**-0.5 * math.log2(math.e)
MESH = pl.DeviceIdType.MESH
CHUNK = 8


def dot_t(a, b):
    return lax.dot_general(a, b, (((1,), (1,)), ((), ())), preferred_element_type=jnp.float32)


def dot_n(a, b):
    return lax.dot_general(a, b, (((1,), (0,)), ((), ())), preferred_element_type=jnp.float32)


DIRS = {"y+": (0, 1), "y-": (0, -1), "z+": (1, 0), "z-": (-1, 0)}


def plan():
    moves, waits = [], []

    def add(dz, dy, x0, nx, way):
        moves.append((dz, dy, x0, nx, way))
        return len(moves) - 1

    steps = []
    own = {w: add(0, 0, 0, 4, w) for w in ("y-", "z-", "z+", "y+")}
    steps.append(([], list(own.values())))
    up = [add(0, 1, 0, 4, "y-"), add(0, 1, 0, 2, "z+"), add(0, 1, 0, 2, "z-")]
    steps.append(([own["y-"]], up))
    zu = [add(1, 0, 2, 1, "z-"), add(1, 0, 0, 1, "z-"), add(1, 0, 2, 2, "y-"), add(1, 0, 2, 2, "y+")]
    steps.append(([own["z-"]], zu))
    zd = [add(-1, 0, 3, 1, "z+"), add(-1, 0, 1, 1, "z+"), add(-1, 0, 2, 2, "y-"), add(-1, 0, 2, 2, "y+")]
    steps.append(([own["z+"]], zd))
    dn = [add(0, -1, 0, 2, "z+"), add(0, -1, 0, 2, "z-")]
    steps.append(([own["y+"]], dn))
    z2 = [add(2, 0, 2, 2, "y-"), add(2, 0, 2, 2, "y+")]
    steps.append(([zu[0], zd[0]], z2))
    y2 = [add(0, 2, 0, 2, "z+"), add(0, 2, 0, 2, "z-")]
    steps.append(([up[0]], y2))
    a_in = {1: (up[1], up[2]), -1: (dn[0], dn[1]), 2: (y2[0], y2[1])}
    b_in = {1: (zu[2], zu[3]), -1: (zd[2], zd[3]), 2: (z2[0], z2[1])}
    last = [zu[1], zd[1]]
    for d in (1, -1, 2):
        plus, minus = a_in[d]
        f = add(1, d, 0, 1, "z-")
        steps.append(([minus], [f]))
        g = add(-1, d, 1, 1, "z+")
        steps.append(([plus], [g]))
        bm, bp = b_in[d]
        h = add(d, 1, 2, 2, "y-")
        steps.append(([bm], [h]))
        last += [f, g, h, bp]
    steps.append((last, []))
    return moves, steps


MOVES, STEPS = plan()


def exchange_kernel(
    vert, slash, q_ref, k_ref, v_ref, kv_out, qx_out, ol_ref, ll_ref,
    kvb, qx, sel, prev, bias,
    x_send, x_recv, q_send, q_recv, p_send, p_recv, m_send, m_recv, out_sem,
):
    s = lax.axis_index("seq")
    core = lax.axis_index("head")
    x, z, y = s // 16, (s // 4) % 4, s % 4
    p = s % 16

    def at(ax, az, ay):
        return (ax % 4) * 16 + (az % 4) * 4 + ay % 4

    right, left = (s + 1) % 64, (s + 63) % 64
    x_peers = [at(x + d, z, y) for d in (1, 2, 3)]
    greet = x_peers + [at(x, z + dz, y + dy) for dz, dy in DIRS.values()] + [right, left]
    barrier = pltpu.get_barrier_semaphore()
    for peer in greet:
        pl.semaphore_signal(barrier, inc=1, device_id=(peer, core), device_id_type=MESH)

    for h in range(KVL):
        def scan(r, found):
            count, first, second = found
            inside = vert[h, r] - s * NB
            here = jnp.where((inside >= 0) & (inside < NB), 1, 0)
            first = first + here * jnp.where(count == 0, inside, 0)
            second = second + here * jnp.where(count == 1, inside, 0)
            return count + here, first, second

        zero = jnp.int32(0)
        unused, first, second = lax.fori_loop(0, NV, scan, (zero, zero, zero), unroll=8)
        cols = slice(h * D, (h + 1) * D)
        for slot, b in enumerate((first, second)):
            for far, ref in ((0, k_ref), (2, v_ref)):
                picked = jnp.zeros((BLK, D), jnp.float32)
                for i in range(NB):
                    block = ref[i * BLK : (i + 1) * BLK, cols].astype(jnp.float32)
                    picked = picked + block * jnp.where(b == i, 1.0, 0.0)
                sel[h, far + slot] = picked.astype(jnp.bfloat16)
    kvb[p, x] = sel[x]
    pl.semaphore_wait(barrier, len(greet))

    def remote(src, dst, a, b, peer):
        return pltpu.make_async_remote_copy(
            src_ref=src, dst_ref=dst, send_sem=a, recv_sem=b,
            device_id=(peer, core), device_id_type=MESH,
        )

    x_copies = [
        remote(sel.at[(x + d) % 4], kvb.at[p, x], x_send.at[d - 1], x_recv.at[d - 1], x_peers[d - 1])
        for d in (1, 2, 3)
    ]
    for d in (2, 1, 3):
        x_copies[d - 1].start()
    p_copies = [
        remote(ref, prev.at[i], p_send.at[i], p_recv.at[i], right)
        for i, ref in enumerate((k_ref, v_ref))
    ]
    p_copies[0].start()
    q_copies = [
        remote(
            q_ref.at[:, pl.ds(pl.multiple_of(((x + d) % 4) * (G * D), G * D), G * D)],
            qx.at[x], q_send.at[d - 1], q_recv.at[d - 1], x_peers[d - 1],
        )
        for d in (1, 2, 3)
    ]
    for d in (2, 1, 3):
        q_copies[d - 1].start()
    qx[x] = q_ref[:, pl.ds(pl.multiple_of(x * (G * D), G * D), G * D)]

    moves = []
    for i, (dz, dy, x0, nx, way) in enumerate(MOVES):
        wz, wy = DIRS[way]
        piece = kvb.at[((z + dz) % 4) * 4 + (y + dy) % 4, pl.ds(x0, nx)]
        moves.append(remote(piece, piece, m_send.at[i], m_recv.at[i], at(x, z + wz, y + wy)))

    key_block = lax.broadcasted_iota(jnp.int32, (8, 2 * ROWS), 1) // BLK
    block_id = key_block + (s - 1) * NB
    for h in range(KVL):
        def mark(r, seen):
            return seen | jnp.where(block_id == vert[h, r], 1, 0)

        seen = lax.fori_loop(0, NV, mark, jnp.zeros((8, 2 * ROWS), jnp.int32), unroll=8)
        gap = lax.broadcasted_iota(jnp.int32, (8, 2 * ROWS), 0) + NB - key_block
        near = (gap == 0) | (gap == slash[h, 0]) | (gap == slash[h, 1]) | (seen > 0)
        ok = near & (gap >= 0) & (block_id >= 0)
        bias[h] = jnp.where(ok, 0.0, NEG)

    def local_unit(h, a):
        keys = 2 * ROWS if a >= 2 else ROWS + 2 * BLK
        own_keys = keys - ROWS
        cols = slice(h * D, (h + 1) * D)
        rows = slice(a * BLK, (a + 1) * BLK)
        q = jnp.concatenate(
            [q_ref[rows, (h * G + g) * D : (h * G + g + 1) * D] for g in range(G)], axis=0
        )
        ks = jnp.concatenate([prev[0, :, cols], k_ref[:own_keys, cols]], axis=0)
        vs = jnp.concatenate([prev[1, :, cols], v_ref[:own_keys, cols]], axis=0)
        t = lax.broadcasted_iota(jnp.int32, (G * BLK, keys), 0) % BLK + (ROWS + a * BLK)
        u = lax.broadcasted_iota(jnp.int32, (G * BLK, keys), 1)
        scores = dot_t(q, ks) + bias[h, a : a + 1, :keys]
        scores = jnp.where(u <= t, scores, NEG)
        top = jnp.max(scores, axis=1, keepdims=True)
        weights = jnp.exp2((scores - top) * C2)
        total = jnp.sum(weights, axis=1, keepdims=True)
        out = dot_n(weights.astype(jnp.bfloat16), vs) / total
        level = top * C2 + jnp.log2(total)
        lane = lax.broadcasted_iota(jnp.int32, (BLK, D), 1)
        levels = ll_ref[rows, :] if h else jnp.zeros((BLK, D), jnp.float32)
        for g in range(G):
            part = slice(g * BLK, (g + 1) * BLK)
            ol_ref[rows, (h * G + g) * D : (h * G + g + 1) * D] = out[part]
            levels = jnp.where(lane == h * G + g, level[part], levels)
        ll_ref[rows, :] = levels

    units = [(h, a) for a in range(NB) for h in range(KVL)]

    for c in x_copies:
        c.wait_recv()
    for i, (need, begin) in enumerate(STEPS):
        for w in need:
            moves[w].wait_recv()
        for w in begin:
            moves[w].start()
        if i == 0:
            p_copies[1].start()
        if i == 6:
            for c in p_copies:
                c.wait_recv()
        if i >= 6:
            for unused in range(2):
                if units:
                    local_unit(*units.pop(0))
    while units:
        local_unit(*units.pop(0))
    for c in q_copies:
        c.wait_recv()
    outs = [
        pltpu.make_async_copy(kvb, kv_out, out_sem.at[0]),
        pltpu.make_async_copy(qx, qx_out, out_sem.at[1]),
    ]
    for c in outs:
        c.start()
    for c in x_copies + q_copies + p_copies + moves:
        c.wait_send()
    for c in outs:
        c.wait()


def exchange(vertical, slash, queries, keys, values):
    bf16, f32 = jnp.bfloat16, jnp.float32
    vmem = pl.BlockSpec(memory_space=pltpu.VMEM)
    smem = pl.BlockSpec(memory_space=pltpu.SMEM)
    hbm = pl.BlockSpec(memory_space=pl.ANY)
    dma = pltpu.SemaphoreType.DMA
    n = len(MOVES)
    return pl.pallas_call(
        exchange_kernel,
        out_shape=(
            jax.ShapeDtypeStruct((PLANE, RING, 2 * CAP, BLK, D), bf16),
            jax.ShapeDtypeStruct((RING, ROWS, G * D), bf16),
            jax.ShapeDtypeStruct((ROWS, KVL * G * D), f32),
            jax.ShapeDtypeStruct((ROWS, D), f32),
        ),
        in_specs=[smem, smem, vmem, vmem, vmem],
        out_specs=(hbm, hbm, vmem, vmem),
        scratch_shapes=[
            pltpu.VMEM((PLANE, RING, 2 * CAP, BLK, D), bf16),
            pltpu.VMEM((RING, ROWS, G * D), bf16),
            pltpu.VMEM((RING, 2 * CAP, BLK, D), bf16),
            pltpu.VMEM((2, ROWS, KVL * D), bf16),
            pltpu.VMEM((KVL, 8, 2 * ROWS), f32),
            dma((3,)), dma((3,)), dma((3,)), dma((3,)), dma((2,)), dma((2,)),
            dma((n,)), dma((n,)), dma((2,)),
        ],
        compiler_params=pltpu.CompilerParams(collective_id=0, has_side_effects=True),
        name="exchange",
    )(vertical, slash, queries, keys, values)


def vertical_kernel(vert, kv_ref, qx_ref, ov_ref, lv_ref, kc, vc, m_ref, l_ref, acc, sems):
    s = lax.axis_index("seq")
    x, p = s // 16, s % 16
    step = CHUNK * BLK

    def fetch(r):
        b = vert[x, r]
        slab = b // NB
        before = vert[x, jnp.maximum(r - 1, 0)] // NB
        slot = jnp.where((r > 0) & (before == slab), 1, 0)
        rows = pl.ds(pl.multiple_of(r * BLK, BLK), BLK)
        src = kv_ref.at[slab % 16, slab // 16]
        return (
            pltpu.make_async_copy(src.at[slot], kc.at[rows], sems.at[0, r // CHUNK]),
            pltpu.make_async_copy(src.at[2 + slot], vc.at[rows], sems.at[1, r // CHUNK]),
        )

    def begin(r, unused):
        for c in fetch(r):
            c.start()
        return unused

    lax.fori_loop(0, NV, begin, 0)

    def count(i):
        limit = (i * 16 + p - 1) * NB
        return lax.fori_loop(
            0, NV, lambda r, n: n + jnp.where(vert[x, r] < limit, 1, 0), jnp.int32(0), unroll=8
        )

    for c in range(NV // CHUNK):
        rows = pl.ds(c * step, step)
        pltpu.make_async_copy(kc.at[rows], kc.at[rows], sems.at[0, c]).wait()
        pltpu.make_async_copy(vc.at[rows], vc.at[rows], sems.at[1, c]).wait()

    def slab_step(i, unused):
        n = count(i)
        full = n // CHUNK
        m_ref[...] = jnp.full(m_ref.shape, NEG, jnp.float32)
        l_ref[...] = jnp.zeros(l_ref.shape, jnp.float32)
        acc[...] = jnp.zeros(acc.shape, jnp.float32)

        def chunk(c, masked):
            rows = pl.ds(pl.multiple_of(c * step, step), step)
            ks, vs = kc[rows, :], vc[rows, :]
            for g in range(G):
                q = qx_ref[i, :, g * D : (g + 1) * D]
                scores = dot_t(q, ks)
                if masked:
                    u = lax.broadcasted_iota(jnp.int32, (1, step), 1) + c * step
                    scores = jnp.where(u < n * BLK, scores, NEG)
                old = m_ref[g]
                top = jnp.maximum(old, jnp.max(scores, axis=1, keepdims=True))
                shrink = jnp.exp2((old - top) * C2)
                weights = jnp.exp2((scores - top[:, :1]) * C2)
                l_ref[g] = l_ref[g] * shrink + jnp.sum(weights, axis=1, keepdims=True)
                acc[g] = acc[g] * shrink + dot_n(weights.astype(jnp.bfloat16), vs)
                m_ref[g] = top

        lax.fori_loop(0, full, lambda c, u: (chunk(c, False), u)[1], 0)

        @pl.when(full * CHUNK < n)
        def _():
            chunk(full, True)

        lane = lax.broadcasted_iota(jnp.int32, (ROWS, D), 1)
        levels = jnp.full((ROWS, D), NEG, jnp.float32)
        for g in range(G):
            total = l_ref[g]
            some = total > 0.0
            safe = jnp.where(some, total, 1.0)
            ov_ref[i, :, g * D : (g + 1) * D] = (acc[g] / safe).astype(jnp.bfloat16)
            level = jnp.where(some, m_ref[g] * C2 + jnp.log2(safe), NEG)
            levels = jnp.where(lane == g, level, levels)
        lv_ref[i] = levels.T[:8, :]
        return unused

    lax.fori_loop(0, RING, slab_step, 0)


def vertical_part(vertical, kv, qx):
    bf16, f32 = jnp.bfloat16, jnp.float32
    vmem = pl.BlockSpec(memory_space=pltpu.VMEM)
    return pl.pallas_call(
        vertical_kernel,
        out_shape=(
            jax.ShapeDtypeStruct((RING, ROWS, G * D), bf16),
            jax.ShapeDtypeStruct((RING, 8, ROWS), f32),
        ),
        in_specs=[
            pl.BlockSpec(memory_space=pltpu.SMEM), pl.BlockSpec(memory_space=pl.ANY), vmem,
        ],
        out_specs=(vmem, vmem),
        scratch_shapes=[
            pltpu.VMEM((NV * BLK, D), bf16),
            pltpu.VMEM((NV * BLK, D), bf16),
            pltpu.VMEM((G, ROWS, D), f32),
            pltpu.VMEM((G, ROWS, D), f32),
            pltpu.VMEM((G, ROWS, D), f32),
            pltpu.SemaphoreType.DMA((2, NV // CHUNK)),
        ],
        name="verticals",
    )(vertical, kv, qx)


def project_kernel(
    ov_ref, lv_ref, ol_ref, ll_ref, w_hbm, out_ref,
    w, ovb, lvb, att, acc, give, take,
    w_sem, o_send, o_recv, l_send, l_recv, c_send, c_recv,
):
    s = lax.axis_index("seq")
    core = lax.axis_index("head")
    x, p = s // 16, s % 16
    peers = [((x + d) % 4) * 16 + p for d in (1, 2, 3)]
    barrier = pltpu.get_barrier_semaphore()
    for peer in peers:
        pl.semaphore_signal(barrier, inc=1, device_id=(peer, core), device_id_type=MESH)
    pl.semaphore_signal(barrier, inc=1, device_id=(s, 1 - core), device_id_type=MESH)

    order = [(x + d) % 4 for d in (0, 1, 3, 2)]
    w_copies = []
    for i, h in enumerate(order):
        rows = pl.ds(pl.multiple_of(h * (G * D), G * D), G * D)
        c = pltpu.make_async_copy(w_hbm.at[rows], w.at[i], w_sem.at[i])
        c.start()
        w_copies.append(c)
    pl.semaphore_wait(barrier, 4)

    def remote(src, dst, a, b, peer):
        return pltpu.make_async_remote_copy(
            src_ref=src, dst_ref=dst, send_sem=a, recv_sem=b,
            device_id=peer, device_id_type=MESH,
        )

    copies = {}
    for d in (2, 1, 3):
        to = (x + d) % 4
        copies[d] = (
            remote(lv_ref.at[to], lvb.at[x], l_send.at[d - 1], l_recv.at[d - 1], (peers[d - 1], core)),
            remote(ov_ref.at[to], ovb.at[x], o_send.at[d - 1], o_recv.at[d - 1], (peers[d - 1], core)),
        )
        for c in copies[d]:
            c.start()

    def merge(h, ov, lv):
        level = jnp.concatenate([lv, jnp.full((D - 8, ROWS), NEG, jnp.float32)], axis=0).T
        base = ll_ref[...]
        lane = lax.broadcasted_iota(jnp.int32, (ROWS, D), 1)
        for g in range(G):
            mine = jnp.sum(jnp.where(lane == h * G + g, base, 0.0), axis=1, keepdims=True)
            far = level[:, g : g + 1]
            share = 1.0 / (1.0 + jnp.exp2(far - mine))
            cols = pl.ds(pl.multiple_of((h * G + g) * D, D), D)
            v = ov[:, g * D : (g + 1) * D].astype(jnp.float32)
            mixed = ol_ref[:, cols] * share + v * (1.0 - share)
            att[:, g * D : (g + 1) * D] = mixed.astype(jnp.bfloat16)

    tile = 512

    def part(i, rows, cols):
        return dot_n(att[rows, :], w[i, :, cols])

    everything = pl.ds(0, ROWS)
    for i, d in enumerate((0, 1, 3)):
        h = order[i]
        if d == 0:
            merge(h, ov_ref[x], lv_ref[x])
        else:
            for c in copies[4 - d]:
                c.wait_recv()
            merge(h, ovb[h], lvb[h])
        w_copies[i].wait()

        @pl.loop(0, OUT // tile)
        def _(t):
            cols = pl.ds(pl.multiple_of(t * tile, tile), tile)
            if i == 0:
                acc[:, cols] = part(i, everything, cols)
            else:
                acc[:, cols] += part(i, everything, cols)

    h = order[3]
    for c in copies[2]:
        c.wait_recv()
    merge(h, ovb[h], lvb[h])
    w_copies[3].wait()
    half = ROWS // 2
    theirs = pl.ds(pl.multiple_of((1 - core) * half, half), half)
    mine = pl.ds(pl.multiple_of(core * half, half), half)
    wide = 1024
    handed = []
    for t in range(OUT // wide):
        cols = pl.ds(t * wide, wide)
        give[t] = (acc[theirs, cols] + part(3, theirs, cols)).astype(jnp.bfloat16)
        c = remote(give.at[t], take.at[t], c_send.at[t], c_recv.at[t], (s, 1 - core))
        c.start()
        handed.append(c)
    for t in range(OUT // wide):
        cols = pl.ds(t * wide, wide)
        total = acc[mine, cols] + part(3, mine, cols)
        handed[t].wait_recv()
        out_ref[:, cols] = (total + take[t].astype(jnp.float32)).astype(jnp.bfloat16)
    for d in (1, 2, 3):
        for c in copies[d]:
            c.wait_send()
    for c in handed:
        c.wait_send()


def project(ov, lv, ol, ll, out_weight):
    bf16, f32 = jnp.bfloat16, jnp.float32
    vmem = pl.BlockSpec(memory_space=pltpu.VMEM)
    dma = pltpu.SemaphoreType.DMA
    return pl.pallas_call(
        project_kernel,
        out_shape=jax.ShapeDtypeStruct((ROWS // 2, OUT), bf16),
        in_specs=[vmem, vmem, vmem, vmem, pl.BlockSpec(memory_space=pl.ANY)],
        out_specs=vmem,
        scratch_shapes=[
            pltpu.VMEM((KVL, G * D, OUT), bf16),
            pltpu.VMEM((RING, ROWS, G * D), bf16),
            pltpu.VMEM((RING, 8, ROWS), f32),
            pltpu.VMEM((ROWS, G * D), bf16),
            pltpu.VMEM((ROWS, OUT), f32),
            pltpu.VMEM((4, ROWS // 2, 1024), bf16),
            pltpu.VMEM((4, ROWS // 2, 1024), bf16),
            dma((4,)), dma((3,)), dma((3,)), dma((3,)), dma((3,)), dma((4,)), dma((4,)),
        ],
        compiler_params=pltpu.CompilerParams(collective_id=1, has_side_effects=True),
        name="project",
    )(ov, lv, ol, ll, out_weight)


def on_device(queries, keys, values, vertical, slash, out_weight):
    kv, qx, ol, ll = exchange(vertical, slash, queries, keys, values)
    ov, lv = vertical_part(vertical, kv, qx)
    return project(ov, lv, ol, ll, out_weight)


def solution(mesh):
    placed = (
        P("seq", "head"),
        P("seq", "head"),
        P("seq", "head"),
        P("head", None),
        P("head", None),
        P("head", None),
    )
    return jax.shard_map(
        on_device, mesh=mesh, in_specs=placed, out_specs=P(("seq", "head"), None), check_vma=False
    )
```

```python
import functools
import math

import jax
import jax.numpy as jnp
from jax import lax
from jax.experimental import pallas as pl
from jax.experimental.pallas import tpu as pltpu
from jax.sharding import PartitionSpec as P

D = 128
BLK = 64
CAP = 2
KVL = 4
G = 4
ROWS = 256
NB = 4
RING = 4
PLANE = 16
NV = 64
OUT = 4096
NEG = -1e30
C2 = D**-0.5 * math.log2(math.e)
MESH = pl.DeviceIdType.MESH
CHUNK = 16
STEP = CHUNK * BLK
FETCH = 8
TALL = 2
TALL_ROWS = TALL * ROWS


def dot_t(a, b):
    return lax.dot_general(a, b, (((1,), (1,)), ((), ())), preferred_element_type=jnp.float32)


def dot_n(a, b):
    return lax.dot_general(a, b, (((1,), (0,)), ((), ())), preferred_element_type=jnp.float32)


DIRS = {"y+": (0, 1), "y-": (0, -1), "z+": (1, 0), "z-": (-1, 0)}


def plan():
    moves, waits = [], []

    def add(dz, dy, x0, nx, way):
        moves.append((dz, dy, x0, nx, way))
        return len(moves) - 1

    steps = []
    own = {w: add(0, 0, 0, 4, w) for w in ("y-", "z-", "z+", "y+")}
    steps.append(([], list(own.values())))
    up = [add(0, 1, 0, 4, "y-"), add(0, 1, 0, 2, "z+"), add(0, 1, 0, 2, "z-")]
    steps.append(([own["y-"]], up))
    zu = [add(1, 0, 2, 1, "z-"), add(1, 0, 0, 1, "z-"), add(1, 0, 2, 2, "y-"), add(1, 0, 2, 2, "y+")]
    steps.append(([own["z-"]], zu))
    zd = [add(-1, 0, 3, 1, "z+"), add(-1, 0, 1, 1, "z+"), add(-1, 0, 2, 2, "y-"), add(-1, 0, 2, 2, "y+")]
    steps.append(([own["z+"]], zd))
    dn = [add(0, -1, 0, 2, "z+"), add(0, -1, 0, 2, "z-")]
    steps.append(([own["y+"]], dn))
    z2 = [add(2, 0, 2, 2, "y-"), add(2, 0, 2, 2, "y+")]
    steps.append(([zu[0], zd[0]], z2))
    y2 = [add(0, 2, 0, 2, "z+"), add(0, 2, 0, 2, "z-")]
    steps.append(([up[0]], y2))
    a_in = {1: (up[1], up[2]), -1: (dn[0], dn[1]), 2: (y2[0], y2[1])}
    b_in = {1: (zu[2], zu[3]), -1: (zd[2], zd[3]), 2: (z2[0], z2[1])}
    last = [zu[1], zd[1]]
    for d in (1, -1, 2):
        plus, minus = a_in[d]
        f = add(1, d, 0, 1, "z-")
        steps.append(([minus], [f]))
        g = add(-1, d, 1, 1, "z+")
        steps.append(([plus], [g]))
        bm, bp = b_in[d]
        h = add(d, 1, 2, 2, "y-")
        steps.append(([bm], [h]))
        last += [f, g, h, bp]
    steps.append((last, []))
    return moves, steps


MOVES, STEPS = plan()


def exchange_kernel(
    vert, slash, q_ref, k_ref, v_ref, kv_out, qx_out, ol_ref, ll_ref,
    kvb, qx, sel, prev, bias,
    x_send, x_recv, q_send, q_recv, p_send, p_recv, m_send, m_recv, out_sem,
):
    s = lax.axis_index("seq")
    core = lax.axis_index("head")
    x, z, y = s // 16, (s // 4) % 4, s % 4
    p = s % 16

    def at(ax, az, ay):
        return (ax % 4) * 16 + (az % 4) * 4 + ay % 4

    right, left = (s + 1) % 64, (s + 63) % 64
    x_peers = [at(x + d, z, y) for d in (1, 2, 3)]
    greet = x_peers + [at(x, z + dz, y + dy) for dz, dy in DIRS.values()] + [right, left]
    barrier = pltpu.get_barrier_semaphore()
    for peer in greet:
        pl.semaphore_signal(barrier, inc=1, device_id=(peer, core), device_id_type=MESH)

    for h in range(KVL):
        def scan(r, found):
            count, first, second = found
            inside = vert[h, r] - s * NB
            here = jnp.where((inside >= 0) & (inside < NB), 1, 0)
            first = first + here * jnp.where(count == 0, inside, 0)
            second = second + here * jnp.where(count == 1, inside, 0)
            return count + here, first, second

        zero = jnp.int32(0)
        unused, first, second = lax.fori_loop(0, NV, scan, (zero, zero, zero), unroll=8)
        cols = slice(h * D, (h + 1) * D)
        for slot, b in enumerate((first, second)):
            for far, ref in ((0, k_ref), (2, v_ref)):
                picked = jnp.zeros((BLK, D), jnp.float32)
                for i in range(NB):
                    block = ref[i * BLK : (i + 1) * BLK, cols].astype(jnp.float32)
                    picked = picked + block * jnp.where(b == i, 1.0, 0.0)
                sel[h, far + slot] = picked.astype(jnp.bfloat16)
    kvb[p, x] = sel[x]
    pl.semaphore_wait(barrier, len(greet))

    def remote(src, dst, a, b, peer):
        return pltpu.make_async_remote_copy(
            src_ref=src, dst_ref=dst, send_sem=a, recv_sem=b,
            device_id=(peer, core), device_id_type=MESH,
        )

    x_copies = [
        remote(sel.at[(x + d) % 4], kvb.at[p, x], x_send.at[d - 1], x_recv.at[d - 1], x_peers[d - 1])
        for d in (1, 2, 3)
    ]
    for d in (2, 1, 3):
        x_copies[d - 1].start()
    p_copies = [
        remote(ref, prev.at[i], p_send.at[i], p_recv.at[i], right)
        for i, ref in enumerate((k_ref, v_ref))
    ]
    p_copies[0].start()
    q_copies = [
        remote(
            q_ref.at[:, pl.ds(pl.multiple_of(((x + d) % 4) * (G * D), G * D), G * D)],
            qx.at[x], q_send.at[d - 1], q_recv.at[d - 1], x_peers[d - 1],
        )
        for d in (1, 2, 3)
    ]
    for d in (2, 1, 3):
        q_copies[d - 1].start()
    qx[x] = q_ref[:, pl.ds(pl.multiple_of(x * (G * D), G * D), G * D)]

    moves = []
    for i, (dz, dy, x0, nx, way) in enumerate(MOVES):
        wz, wy = DIRS[way]
        piece = kvb.at[((z + dz) % 4) * 4 + (y + dy) % 4, pl.ds(x0, nx)]
        moves.append(remote(piece, piece, m_send.at[i], m_recv.at[i], at(x, z + wz, y + wy)))

    key_block = lax.broadcasted_iota(jnp.int32, (8, 2 * ROWS), 1) // BLK
    block_id = key_block + (s - 1) * NB
    for h in range(KVL):
        def mark(r, seen):
            return seen | jnp.where(block_id == vert[h, r], 1, 0)

        seen = lax.fori_loop(0, NV, mark, jnp.zeros((8, 2 * ROWS), jnp.int32), unroll=8)
        gap = lax.broadcasted_iota(jnp.int32, (8, 2 * ROWS), 0) + NB - key_block
        near = (gap == 0) | (gap == slash[h, 0]) | (gap == slash[h, 1]) | (seen > 0)
        ok = near & (gap >= 0) & (block_id >= 0)
        bias[h] = jnp.where(ok, 0.0, NEG)

    def local_unit(h, a):
        keys = 2 * ROWS if a >= 2 else ROWS + 2 * BLK
        own_keys = keys - ROWS
        cols = slice(h * D, (h + 1) * D)
        rows = slice(a * BLK, (a + 1) * BLK)
        q = jnp.concatenate(
            [q_ref[rows, (h * G + g) * D : (h * G + g + 1) * D] for g in range(G)], axis=0
        )
        ks = jnp.concatenate([prev[0, :, cols], k_ref[:own_keys, cols]], axis=0)
        vs = jnp.concatenate([prev[1, :, cols], v_ref[:own_keys, cols]], axis=0)
        t = lax.broadcasted_iota(jnp.int32, (G * BLK, keys), 0) % BLK + (ROWS + a * BLK)
        u = lax.broadcasted_iota(jnp.int32, (G * BLK, keys), 1)
        scores = dot_t(q, ks) + bias[h, a : a + 1, :keys]
        scores = jnp.where(u <= t, scores, NEG)
        top = jnp.max(scores, axis=1, keepdims=True)
        weights = jnp.exp2((scores - top) * C2)
        total = jnp.sum(weights, axis=1, keepdims=True)
        out = dot_n(weights.astype(jnp.bfloat16), vs) / total
        level = top * C2 + jnp.log2(total)
        lane = lax.broadcasted_iota(jnp.int32, (BLK, D), 1)
        levels = ll_ref[rows, :] if h else jnp.zeros((BLK, D), jnp.float32)
        for g in range(G):
            part = slice(g * BLK, (g + 1) * BLK)
            ol_ref[rows, (h * G + g) * D : (h * G + g + 1) * D] = out[part]
            levels = jnp.where(lane == h * G + g, level[part], levels)
        ll_ref[rows, :] = levels

    units = [(h, a) for a in range(NB) for h in range(KVL)]

    for c in x_copies:
        c.wait_recv()
    for i, (need, begin) in enumerate(STEPS):
        for w in need:
            moves[w].wait_recv()
        for w in begin:
            moves[w].start()
        if i == 0:
            p_copies[1].start()
        if i == 6:
            for c in p_copies:
                c.wait_recv()
        if i >= 6:
            for unused in range(2):
                if units:
                    local_unit(*units.pop(0))
    while units:
        local_unit(*units.pop(0))
    for c in q_copies:
        c.wait_recv()
    outs = [
        pltpu.make_async_copy(kvb, kv_out, out_sem.at[0]),
        pltpu.make_async_copy(qx, qx_out, out_sem.at[1]),
    ]
    for c in outs:
        c.start()
    for c in x_copies + q_copies + p_copies + moves:
        c.wait_send()
    for c in outs:
        c.wait()


def exchange(vertical, slash, queries, keys, values):
    bf16, f32 = jnp.bfloat16, jnp.float32
    vmem = pl.BlockSpec(memory_space=pltpu.VMEM)
    smem = pl.BlockSpec(memory_space=pltpu.SMEM)
    hbm = pl.BlockSpec(memory_space=pl.ANY)
    dma = pltpu.SemaphoreType.DMA
    n = len(MOVES)
    return pl.pallas_call(
        exchange_kernel,
        out_shape=(
            jax.ShapeDtypeStruct((PLANE, RING, 2 * CAP, BLK, D), bf16),
            jax.ShapeDtypeStruct((RING, ROWS, G * D), bf16),
            jax.ShapeDtypeStruct((ROWS, KVL * G * D), f32),
            jax.ShapeDtypeStruct((ROWS, D), f32),
        ),
        in_specs=[smem, smem, vmem, vmem, vmem],
        out_specs=(hbm, hbm, vmem, vmem),
        scratch_shapes=[
            pltpu.VMEM((PLANE, RING, 2 * CAP, BLK, D), bf16),
            pltpu.VMEM((RING, ROWS, G * D), bf16),
            pltpu.VMEM((RING, 2 * CAP, BLK, D), bf16),
            pltpu.VMEM((2, ROWS, KVL * D), bf16),
            pltpu.VMEM((KVL, 8, 2 * ROWS), f32),
            dma((3,)), dma((3,)), dma((3,)), dma((3,)), dma((2,)), dma((2,)),
            dma((n,)), dma((n,)), dma((2,)),
        ],
        compiler_params=pltpu.CompilerParams(collective_id=0, has_side_effects=True),
        name="exchange",
    )(vertical, slash, queries, keys, values)


def vertical_kernel(
    vert, kv_ref, qx_ref, ov_ref, lv_ref,
    kc, vc, qt, m_ref, l_ref, acc, s0, s1, x0, x1, todo, sems, q_sem,
):
    s = lax.axis_index("seq")
    x, p = s // 16, s % 16
    q_copies = []
    for i in range(RING):
        for g in range(G):
            c = pltpu.make_async_copy(
                qx_ref.at[i, :, g * D : (g + 1) * D],
                qt.at[pl.ds((i * G + g) * ROWS, ROWS)],
                q_sem.at[i * G + g],
            )
            c.start()
            q_copies.append(c)

    def begin(r, unused):
        b = vert[x, r]
        slab = b // NB
        before = vert[x, jnp.maximum(r - 1, 0)] // NB
        slot = jnp.where((r > 0) & (before == slab), 1, 0)
        rows = pl.ds(pl.multiple_of(r * BLK, BLK), BLK)
        src = kv_ref.at[slab % 16, slab // 16]
        pltpu.make_async_copy(src.at[slot], kc.at[rows], sems.at[0, r // FETCH]).start()
        pltpu.make_async_copy(src.at[2 + slot], vc.at[rows], sems.at[1, r // FETCH]).start()
        return unused

    lax.fori_loop(0, NV, begin, 0)
    m_ref[...] = jnp.full(m_ref.shape, NEG, jnp.float32)
    l_ref[...] = jnp.zeros(l_ref.shape, jnp.float32)
    acc[...] = jnp.zeros(acc.shape, jnp.float32)

    steps = jnp.int32(0)
    for i in range(RING):
        limit = (i * 16 + p - 1) * NB
        n = lax.fori_loop(
            0, NV, lambda r, n: n + jnp.where(vert[x, r] < limit, 1, 0), jnp.int32(0), unroll=16
        )

        def put(c, t):
            for u in range(G // TALL):
                todo[t + u, 0] = (i * G + u * TALL) * ROWS
                todo[t + u, 1] = c * STEP
                todo[t + u, 2] = n * BLK - c * STEP
            return t + G // TALL

        steps = lax.fori_loop(0, (n + CHUNK - 1) // CHUNK, put, steps)
    for e in range(2):
        todo[steps + e, 0] = RING * G * ROWS
        todo[steps + e, 1] = 0
        todo[steps + e, 2] = STEP

    for c in q_copies:
        c.wait()
    for c in range(NV // FETCH):
        rows = pl.ds(c * FETCH * BLK, FETCH * BLK)
        pltpu.make_async_copy(kc.at[rows], kc.at[rows], sems.at[0, c]).wait()
        pltpu.make_async_copy(vc.at[rows], vc.at[rows], sems.at[1, c]).wait()

    lanes = lax.broadcasted_iota(jnp.int32, (1, STEP), 1)

    def score(t, s_ref, x_ref):
        row, key = pl.multiple_of(todo[t, 0], ROWS), pl.multiple_of(todo[t, 1], STEP)
        scores = dot_t(qt[pl.ds(row, TALL_ROWS), :], kc[pl.ds(key, STEP), :])
        scores = jnp.where(lanes < todo[t, 2], scores, NEG)
        s_ref[...] = scores
        top = scores[:, :D]
        for k in range(1, STEP // D):
            top = jnp.maximum(top, scores[:, k * D : (k + 1) * D])
        x_ref[...] = jnp.broadcast_to(jnp.max(top, axis=1, keepdims=True), (TALL_ROWS, D))

    def weigh(t, s_ref, x_ref):
        row, key = pl.multiple_of(todo[t, 0], ROWS), pl.multiple_of(todo[t, 1], STEP)
        r = pl.ds(row, TALL_ROWS)
        old = m_ref[r, :]
        top = jnp.maximum(old, x_ref[...])
        shrink = jnp.exp2((old - top) * C2)
        rounded, sums = [], None
        for k in range(STEP // D):
            w = jnp.exp2((s_ref[:, k * D : (k + 1) * D] - top) * C2)
            sums = w if sums is None else sums + w
            rounded.append(w.astype(jnp.bfloat16))
        l_ref[r, :] = l_ref[r, :] * shrink + sums
        acc[r, :] = acc[r, :] * shrink + dot_n(
            jnp.concatenate(rounded, axis=1), vc[pl.ds(key, STEP), :]
        )
        m_ref[r, :] = top

    @pl.when(steps > 0)
    def _():
        score(0, s0, x0)

        def pair(h, unused):
            t = 2 * h
            score(t + 1, s1, x1)
            weigh(t, s0, x0)
            score(t + 2, s0, x0)
            weigh(t + 1, s1, x1)
            return unused

        lax.fori_loop(0, (steps + 1) // 2, pair, 0)

    lane = lax.broadcasted_iota(jnp.int32, (ROWS, D), 1)

    def finish(i, unused):
        levels = jnp.full((ROWS, D), NEG, jnp.float32)
        for g in range(G):
            r = pl.ds(pl.multiple_of((i * G + g) * ROWS, ROWS), ROWS)
            total = jnp.sum(l_ref[r, :], axis=1, keepdims=True)
            some = total > 0.0
            safe = jnp.where(some, total, 1.0)
            ov_ref[i, :, g * D : (g + 1) * D] = (acc[r, :] * (1.0 / safe)).astype(jnp.bfloat16)
            level = jnp.where(some, m_ref[r, :] * C2 + jnp.log2(safe), NEG)
            levels = jnp.where(lane == g, level, levels)
        lv_ref[i] = levels.T[:8, :]
        return unused

    lax.fori_loop(0, RING, finish, 0)


def vertical_part(vertical, kv, qx):
    bf16, f32 = jnp.bfloat16, jnp.float32
    vmem = pl.BlockSpec(memory_space=pltpu.VMEM)
    hbm = pl.BlockSpec(memory_space=pl.ANY)
    rows = RING * G * ROWS + TALL_ROWS
    return pl.pallas_call(
        vertical_kernel,
        out_shape=(
            jax.ShapeDtypeStruct((RING, ROWS, G * D), bf16),
            jax.ShapeDtypeStruct((RING, 8, ROWS), f32),
        ),
        in_specs=[pl.BlockSpec(memory_space=pltpu.SMEM), hbm, hbm],
        out_specs=(vmem, vmem),
        scratch_shapes=[
            pltpu.VMEM((NV * BLK, D), bf16),
            pltpu.VMEM((NV * BLK, D), bf16),
            pltpu.VMEM((rows, D), bf16),
            pltpu.VMEM((rows, D), f32),
            pltpu.VMEM((rows, D), f32),
            pltpu.VMEM((rows, D), f32),
            pltpu.VMEM((TALL_ROWS, STEP), f32),
            pltpu.VMEM((TALL_ROWS, STEP), f32),
            pltpu.VMEM((TALL_ROWS, D), f32),
            pltpu.VMEM((TALL_ROWS, D), f32),
            pltpu.SMEM((RING * (G // TALL) * (NV // CHUNK) + 4, 3), jnp.int32),
            pltpu.SemaphoreType.DMA((2, NV // FETCH)),
            pltpu.SemaphoreType.DMA((RING * G,)),
        ],
        name="verticals",
    )(vertical, kv, qx)


def project_kernel(
    ov_ref, lv_ref, ol_ref, ll_ref, w_hbm, out_ref,
    w, ovb, lvb, att, acc, give, take,
    w_sem, o_send, o_recv, l_send, l_recv, c_send, c_recv,
):
    s = lax.axis_index("seq")
    core = lax.axis_index("head")
    x, p = s // 16, s % 16
    peers = [((x + d) % 4) * 16 + p for d in (1, 2, 3)]
    barrier = pltpu.get_barrier_semaphore()
    for peer in peers:
        pl.semaphore_signal(barrier, inc=1, device_id=(peer, core), device_id_type=MESH)
    pl.semaphore_signal(barrier, inc=1, device_id=(s, 1 - core), device_id_type=MESH)

    order = [(x + d) % 4 for d in (0, 1, 3, 2)]
    w_copies = []
    for i, h in enumerate(order):
        rows = pl.ds(pl.multiple_of(h * (G * D), G * D), G * D)
        c = pltpu.make_async_copy(w_hbm.at[rows], w.at[i], w_sem.at[i])
        c.start()
        w_copies.append(c)
    pl.semaphore_wait(barrier, 4)

    def remote(src, dst, a, b, peer):
        return pltpu.make_async_remote_copy(
            src_ref=src, dst_ref=dst, send_sem=a, recv_sem=b,
            device_id=peer, device_id_type=MESH,
        )

    copies = {}
    for d in (2, 1, 3):
        to = (x + d) % 4
        copies[d] = (
            remote(lv_ref.at[to], lvb.at[x], l_send.at[d - 1], l_recv.at[d - 1], (peers[d - 1], core)),
            remote(ov_ref.at[to], ovb.at[x], o_send.at[d - 1], o_recv.at[d - 1], (peers[d - 1], core)),
        )
        for c in copies[d]:
            c.start()

    def merge(h, ov, lv):
        level = jnp.concatenate([lv, jnp.full((D - 8, ROWS), NEG, jnp.float32)], axis=0).T
        base = ll_ref[...]
        lane = lax.broadcasted_iota(jnp.int32, (ROWS, D), 1)
        for g in range(G):
            mine = jnp.sum(jnp.where(lane == h * G + g, base, 0.0), axis=1, keepdims=True)
            far = level[:, g : g + 1]
            share = 1.0 / (1.0 + jnp.exp2(far - mine))
            cols = pl.ds(pl.multiple_of((h * G + g) * D, D), D)
            v = ov[:, g * D : (g + 1) * D].astype(jnp.float32)
            mixed = ol_ref[:, cols] * share + v * (1.0 - share)
            att[:, g * D : (g + 1) * D] = mixed.astype(jnp.bfloat16)

    tile = 512

    def part(i, rows, cols):
        return dot_n(att[rows, :], w[i, :, cols])

    everything = pl.ds(0, ROWS)
    for i, d in enumerate((0, 1, 3)):
        h = order[i]
        if d == 0:
            merge(h, ov_ref[x], lv_ref[x])
        else:
            for c in copies[4 - d]:
                c.wait_recv()
            merge(h, ovb[h], lvb[h])
        w_copies[i].wait()

        @pl.loop(0, OUT // tile)
        def _(t):
            cols = pl.ds(pl.multiple_of(t * tile, tile), tile)
            if i == 0:
                acc[:, cols] = part(i, everything, cols)
            else:
                acc[:, cols] += part(i, everything, cols)

    h = order[3]
    for c in copies[2]:
        c.wait_recv()
    merge(h, ovb[h], lvb[h])
    w_copies[3].wait()
    half = ROWS // 2
    theirs = pl.ds(pl.multiple_of((1 - core) * half, half), half)
    mine = pl.ds(pl.multiple_of(core * half, half), half)
    wide = 1024
    handed = []
    for t in range(OUT // wide):
        cols = pl.ds(t * wide, wide)
        give[t] = (acc[theirs, cols] + part(3, theirs, cols)).astype(jnp.bfloat16)
        c = remote(give.at[t], take.at[t], c_send.at[t], c_recv.at[t], (s, 1 - core))
        c.start()
        handed.append(c)
    for t in range(OUT // wide):
        cols = pl.ds(t * wide, wide)
        total = acc[mine, cols] + part(3, mine, cols)
        handed[t].wait_recv()
        out_ref[:, cols] = (total + take[t].astype(jnp.float32)).astype(jnp.bfloat16)
    for d in (1, 2, 3):
        for c in copies[d]:
            c.wait_send()
    for c in handed:
        c.wait_send()


def project(ov, lv, ol, ll, out_weight):
    bf16, f32 = jnp.bfloat16, jnp.float32
    vmem = pl.BlockSpec(memory_space=pltpu.VMEM)
    dma = pltpu.SemaphoreType.DMA
    return pl.pallas_call(
        project_kernel,
        out_shape=jax.ShapeDtypeStruct((ROWS // 2, OUT), bf16),
        in_specs=[vmem, vmem, vmem, vmem, pl.BlockSpec(memory_space=pl.ANY)],
        out_specs=vmem,
        scratch_shapes=[
            pltpu.VMEM((KVL, G * D, OUT), bf16),
            pltpu.VMEM((RING, ROWS, G * D), bf16),
            pltpu.VMEM((RING, 8, ROWS), f32),
            pltpu.VMEM((ROWS, G * D), bf16),
            pltpu.VMEM((ROWS, OUT), f32),
            pltpu.VMEM((4, ROWS // 2, 1024), bf16),
            pltpu.VMEM((4, ROWS // 2, 1024), bf16),
            dma((4,)), dma((3,)), dma((3,)), dma((3,)), dma((3,)), dma((4,)), dma((4,)),
        ],
        compiler_params=pltpu.CompilerParams(collective_id=1, has_side_effects=True),
        name="project",
    )(ov, lv, ol, ll, out_weight)


def on_device(queries, keys, values, vertical, slash, out_weight):
    kv, qx, ol, ll = exchange(vertical, slash, queries, keys, values)
    ov, lv = vertical_part(vertical, kv, qx)
    return project(ov, lv, ol, ll, out_weight)


def solution(mesh):
    placed = (
        P("seq", "head"),
        P("seq", "head"),
        P("seq", "head"),
        P("head", None),
        P("head", None),
        P("head", None),
    )
    return jax.shard_map(
        on_device, mesh=mesh, in_specs=placed, out_specs=P(("seq", "head"), None), check_vma=False
    )
```
